32 devices in a mesh: expert: 4 (over x, core), tensor: 8 (over z, y).
Axes of the slice: x: 2, y: 2, z: 4, core: 2. Of those that a mesh axis runs over, the one named last changes fastest.
Arguments:
- tokens: bfloat16 [128, 7168], P('expert', 'tensor'), may hold values from -6 to 6
- routes: int32 [128, 8], P('expert'), may hold values from 0 to 15, all different within a row; in each aligned block of 128 rows (0 to 127, 128 to 255, ...) at most 128 rows name the same one
- gates: bfloat16 [128, 8], P('expert'), may hold values from 0.099609375 to 0.59765625
- w_gate: bfloat16 [16, 2048, 7168], P('expert', 'tensor'), may hold values from -0.0625 to 0.0625
- w_up: bfloat16 [16, 2048, 7168], P('expert', 'tensor'), may hold values from -0.0625 to 0.0625
- w_down: bfloat16 [16, 2048, 7168], P('expert', None, 'tensor'), may hold values from -0.125 to 0.125
Outputs:
- moe_out: bfloat16 [128, 7168], P('expert', 'tensor')
The draws below stay inside these ranges and needn't reach their ends.
Inputs may be any that keep to these rules, and one draw needn't show every extreme that they name: `routes`: each row names 8 different experts. No expert is named by more than 128 of the 128 rows, and one expert is named by exactly 128 rows.
All inputs are finite; a program needn't handle non-finite values.
Results may differ from the reference program's by a relative error of at most 0.0049.
Values may be sent and summed in bfloat16 or wider, within the bound.
No kernel may reach another device: no remote copies, remote signals or barrier semaphores. Data moves between devices by JAX's collectives and lax.ppermute only.
A program may use at most 128 MiB of HBM per device.

```python
import math
import jax
import jax.numpy as jnp
import numpy as np
from jax import lax

D = 7168
FF = 2048
TOPK = 8
EXPERTS = 16
TOKENS = 128
CAP = 128


def steps_of(own_key, extent, split, smallest, largest):
    def one(dim, blocks):
        steps = jax.random.uniform(jax.random.fold_in(jax.random.fold_in(own_key, 6), dim), (blocks,), jnp.float32, smallest / len(split), largest / len(split))
        return jnp.repeat(jnp.exp(steps), extent[dim] // blocks).reshape((-1,) + (1,) * (len(extent) - dim - 1))

    factor_of = one(*split[0])
    for cut in split[1:]:
        factor_of = factor_of * one(*cut)
    return factor_of


def shared_out(key, own, number, rows, count, top, limit, lean):
    ranking = jax.random.permutation(key, count)
    crowded, ordinary = load_shares(count, rows * top, limit, lean, True), load_shares(count, rows * top, limit, lean, False)
    places = jnp.arange(count)

    def named(sizes, offset_by):
        used = int((sizes > 0).sum())
        fixed = max(1, used // 4)
        passed = fixed + (places - fixed + offset_by * (used - fixed)) % max(1, count - fixed)
        return jnp.zeros((count,), jnp.int32).at[ranking[jnp.where(places < fixed, places, passed)]].set(jnp.asarray(sizes, jnp.int32))

    sizes = jnp.where(number % 4 == 0, named(crowded, number // 4), named(ordinary, number - number // 4 - 1))
    mixed = jax.random.permutation(jax.random.fold_in(own, 3), count)
    source_of, receiver = mixed[0:count // 2 * 2:2], mixed[1:count // 2 * 2:2]
    room = jnp.minimum(sizes[source_of] - 1, limit - sizes[receiver]) // 2
    room = jnp.where((source_of == ranking[0]) | (receiver == ranking[0]) | (sizes[receiver] == 0), 0, jnp.maximum(room, 0))
    passed = jax.random.randint(jax.random.fold_in(own, 4), (count // 2,), 0, 1 << 20) % (room + 1)
    sizes = sizes.at[source_of].add(-passed).at[receiver].add(passed)
    labels = jnp.searchsorted(jnp.cumsum(sizes), jnp.arange(rows * top), side="right").astype(jnp.int32)
    table = labels.reshape(top, rows).T
    table = table[jax.random.permutation(jax.random.fold_in(own, 1), rows)]
    offset_by = jax.random.randint(jax.random.fold_in(own, 2), (rows, 1), 0, top)
    return jnp.take_along_axis(table, (jnp.arange(top)[None, :] + offset_by) % top, axis=1)


def load_shares(count, total, limit, lean, full):
    weights = [(1 << 20) // math.isqrt(standing ** lean) + 1 for standing in range(1, count + 1)]
    largest = limit if full else min(limit, max(-(-total // count), total * weights[0] // sum(weights)))
    least = 1 if total - largest >= count - 1 else 0
    given, surplus = [largest] + [least] * (count - 1), total - largest - least * (count - 1)
    while surplus > 0:
        movable = [i for i in range(1, count) if given[i] < largest] or [i for i in range(1, count) if given[i] < limit]
        whole, remaining = sum([weights[i] for i in movable]), surplus
        for i in movable:
            more = min(limit - given[i], max(1, remaining * weights[i] // whole), surplus)
            given[i] = given[i] + more
            surplus = surplus - more
    return np.array(given)


def scatter_about(key, shape, width, bound, split=(), kind=jnp.bfloat16):
    values = width * jax.random.normal(key, shape, jnp.float32)
    if split:
        values = values * steps_of(key, shape, split, -0.22, 0.18)
    return jnp.clip(values, -bound, bound).astype(kind)


def setup_inputs(seed: int = 0) -> dict:
    arg_keys = jax.random.split(jax.random.key(seed), 7)
    tokens = scatter_about(arg_keys[0], (TOKENS, D), 1.0, 6.0, ((0, 4), (1, 8)))
    routes_keys = jax.random.split(jax.random.fold_in(arg_keys[1], 1), TOKENS // TOKENS)
    routes_turns = jax.random.permutation(jax.random.fold_in(arg_keys[1], 3), TOKENS // TOKENS)
    routes = jax.vmap(lambda own, number: shared_out(jax.random.fold_in(arg_keys[1], 2), own, number, TOKENS, EXPERTS, TOPK, CAP, 2))(routes_keys, routes_turns).reshape((TOKENS, TOPK))
    gates = jnp.clip(0.099609375 + 0.49804688 * jax.random.uniform(arg_keys[2], (TOKENS, TOPK), jnp.float32) ** steps_of(arg_keys[2], (TOKENS, TOPK), ((0, 4),), -0.2, 0.2), 0.099609375, 0.59765625).astype(jnp.bfloat16)
    w_gate = scatter_about(arg_keys[3], (EXPERTS, FF, D), D ** -0.5, 0.0625, ((0, 4), (1, 8)))
    w_up = scatter_about(arg_keys[4], (EXPERTS, FF, D), D ** -0.5, 0.0625, ((0, 4), (1, 8)))
    w_down = scatter_about(arg_keys[5], (EXPERTS, FF, D), FF ** -0.5, 0.125, ((0, 4), (2, 8)))
    return {"tokens": tokens, "routes": routes, "gates": gates, "w_gate": w_gate, "w_up": w_up, "w_down": w_down}


def reference(tokens, routes, gates, w_gate, w_up, w_down):
    expert_ids = jnp.arange(EXPERTS, dtype=jnp.int32)
    route_hits = routes[:, :, None] == expert_ids[None, None, :]
    member = jnp.sum(route_hits.astype(jnp.int32), axis=1)
    position = jnp.cumsum(member, axis=0) - member
    weights = jnp.sum(gates.astype(jnp.float32)[:, :, None] * route_hits.astype(jnp.float32), axis=1)
    slot_ids = jnp.arange(CAP, dtype=jnp.int32)

    def one_expert(running, packed):
        member_col, place_col, weight_col, gate_w, up_w, down_w = packed
        picked = (place_col[None, :] == slot_ids[:, None]) & (member_col[None, :] > 0)
        slot_rows = jnp.dot(picked.astype(jnp.bfloat16), tokens, preferred_element_type=jnp.float32).astype(jnp.bfloat16)
        gate_proj = lax.dot_general(slot_rows, gate_w, (((1,), (1,)), ((), ())), preferred_element_type=jnp.float32)
        up_proj = lax.dot_general(slot_rows, up_w, (((1,), (1,)), ((), ())), preferred_element_type=jnp.float32)
        hidden = (jax.nn.silu(gate_proj) * up_proj).astype(jnp.bfloat16)
        expert_out = jnp.dot(hidden, down_w, preferred_element_type=jnp.float32)
        mixing = picked.astype(jnp.float32).T * weight_col[:, None]
        return running + jnp.dot(mixing, expert_out, precision=lax.Precision.HIGHEST), None

    start = jnp.zeros((tokens.shape[0], tokens.shape[1]), jnp.float32)
    running, _ = lax.scan(one_expert, start, (member.T, position.T, weights.T, w_gate, w_up, w_down))
    return running.astype(jnp.bfloat16)
```

```python
import functools

import jax
import jax.numpy as jnp
from jax import lax
from jax.experimental import pallas as pl
from jax.experimental.pallas import tpu as pltpu
from jax.sharding import PartitionSpec as P

CAP = 128


def entering(value, axis, combine, identity):
    length, index = (lax.axis_size(axis), lax.axis_index(axis))
    everything = lax.all_gather(value, axis)
    start = jnp.broadcast_to(jnp.asarray(identity, value.dtype), value.shape)

    def lap(k, before):
        reached = k < index
        new = combine(before, everything[k])
        return jnp.where(reached, new, before)

    return lax.fori_loop(0, length, lap, start)


def add_counts(earlier, later):
    return earlier + later


def general(tokens, routes, gates, w_gate, w_up, w_down):
    exp_dev = w_gate.shape[0]
    experts = exp_dev * lax.axis_size("expert")
    group_index = lax.axis_index("expert")
    expert_ids = jnp.arange(experts, dtype=jnp.int32)
    route_hits = routes[:, :, None] == expert_ids[None, None, :]
    member = jnp.sum(route_hits.astype(jnp.int32), axis=1)
    counts = jnp.sum(member, axis=0)
    offset = entering(counts, "expert", add_counts, jnp.zeros_like(counts))
    before = jnp.cumsum(member, axis=0) - member + offset[None, :]
    own_slot = jnp.sum(jnp.where(route_hits, before[:, None, :], 0), axis=2).astype(jnp.int32)
    all_routes, all_slots = (
        lax.all_gather(routes, "expert", axis=0, tiled=True),
        lax.all_gather(own_slot, "expert", axis=0, tiled=True),
    )
    row_block, all_gates = (
        lax.all_gather(tokens, "expert", axis=0, tiled=True),
        lax.all_gather(gates, "expert", axis=0, tiled=True),
    )
    gathered = lax.all_gather(row_block, "tensor", axis=1, tiled=True)
    local_ids = all_routes - group_index * exp_dev
    is_local = (local_ids >= 0) & (local_ids < exp_dev)
    slot_id = jnp.where(is_local, local_ids * CAP + all_slots, -1)
    slot_range = jnp.arange(exp_dev * CAP, dtype=jnp.int32)
    matches = slot_id[:, :, None] == slot_range[None, None, :]
    picked = jnp.any(matches, axis=1).astype(jnp.bfloat16)
    mixing = jnp.sum(jnp.where(matches, all_gates.astype(jnp.float32)[:, :, None], 0.0), axis=1)
    slot_rows = lax.dot_general(
        picked, gathered, (((0,), (0,)), ((), ())), preferred_element_type=jnp.float32
    ).astype(jnp.bfloat16)
    slot_rows = slot_rows.reshape(exp_dev, CAP, gathered.shape[1])
    gate_proj = jnp.einsum("ecd,efd->ecf", slot_rows, w_gate, preferred_element_type=jnp.float32)
    up_proj = jnp.einsum("ecd,efd->ecf", slot_rows, w_up, preferred_element_type=jnp.float32)
    hidden = (jax.nn.silu(gate_proj) * up_proj).astype(jnp.bfloat16)
    expert_out = jnp.einsum(
        "ecf,efd->ecd",
        lax.all_gather(hidden, "tensor", axis=2, tiled=True),
        w_down,
        preferred_element_type=jnp.float32,
    )
    expert_out = expert_out.reshape(exp_dev * CAP, w_down.shape[2])
    partial_value = jnp.dot(mixing, expert_out, precision=lax.Precision.HIGHEST)
    result = lax.psum_scatter(partial_value, "expert", scatter_dimension=0, tiled=True)
    return result.astype(jnp.bfloat16)


COLS = (0, 2, 4, 6, 1, 3, 5, 7)
ROWS = (0, 2, 1, 3)


def swap(value, axis, k):
    n = lax.axis_size(axis)
    return lax.ppermute(value, axis, [(i, i ^ k) for i in range(n)])


def hidden_kernel(at, mine, other, mix, wg, wu, out, x, g_buf, u_buf, sems, *, n_e, width):
    def copies(e):
        return (
            pltpu.make_async_copy(wg.at[e], g_buf.at[e], sems.at[0, e]),
            pltpu.make_async_copy(wu.at[e], u_buf.at[e], sems.at[1, e]),
        )

    for e in range(n_e):
        for c in copies(e):
            c.start()
    half = x.shape[0] // 2
    for j, off in enumerate(COLS):
        col = pl.multiple_of((at[0] ^ off) * width, 128)
        x[0:half, pl.ds(col, width)] = mine[j * half : (j + 1) * half, :]
        x[half:, pl.ds(col, width)] = other[j * half : (j + 1) * half, :]
    dims = (((1,), (1,)), ((), ()))
    for e in range(n_e):
        cg, cu = copies(e)
        cg.wait()
        g = lax.dot_general(x[...], g_buf[e], dims, preferred_element_type=jnp.float32)
        cu.wait()
        u = lax.dot_general(x[...], u_buf[e], dims, preferred_element_type=jnp.float32)
        h = g / (1.0 + jnp.exp(-g)) * u
        out[e] = (h * mix[:, e : e + 1]).astype(jnp.bfloat16)


def down_kernel(at, *refs, n_e, width):
    blocks, (wd, own, away, h, buf, sems) = refs[: len(COLS)], refs[len(COLS) :]

    def copy(e):
        return pltpu.make_async_copy(wd.at[e], buf.at[e], sems.at[e])

    for e in range(n_e):
        copy(e).start()
    for j, off in enumerate(COLS):
        col = pl.multiple_of((at[0] ^ off) * width, 128)
        for e in range(n_e):
            h[e, :, pl.ds(col, width)] = blocks[j][e]
    acc = None
    for e in range(n_e):
        copy(e).wait()
        y = jnp.dot(h[e], buf[e], preferred_element_type=jnp.float32)
        acc = y if acc is None else acc + y
    n = own.shape[0]
    own[...] = acc[:n]
    away[...] = acc[n:].astype(jnp.bfloat16)


def planned(tokens, routes, gates, w_gate, w_up, w_down):
    n_tok, d_dev = tokens.shape
    n_e, f_dev, d_all = w_gate.shape
    f_all = w_down.shape[1]
    experts = n_e * lax.axis_size("expert")
    here = lax.axis_index("expert")
    at = lax.axis_index("tensor").astype(jnp.int32).reshape(1)
    hits = routes[:, :, None] == jnp.arange(experts, dtype=jnp.int32)[None, None, :]
    mix = jnp.sum(jnp.where(hits, gates[:, :, None], jnp.zeros((), gates.dtype)), axis=1)
    mix = jnp.pad(mix, ((0, 0), (0, 128 - experts)))
    first = jnp.concatenate([tokens, mix], axis=1)
    second = swap(first, "expert", 2)
    both = jnp.concatenate([first, second], axis=0)
    block, mix2 = both[:, :d_dev], both[:, d_dev:]
    zs = [swap(block, "tensor", k) for k in (2, 4, 6)]
    ys = [swap(b, "tensor", 1) for b in [block] + zs]
    mix2 = jnp.pad(mix2, ((0, 0), (0, d_dev - 128)))
    mine = jnp.concatenate([block] + zs + ys + [mix2], axis=0)
    other = swap(mine, "expert", 1)
    half = 2 * n_tok
    mix4 = jnp.concatenate([mine[8 * half :, :128], other[8 * half :, :128]], axis=0)
    mix4 = lax.dynamic_slice_in_dim(mix4, here * n_e, n_e, axis=1).astype(jnp.float32)

    vmem = pl.BlockSpec(memory_space=pltpu.VMEM)
    smem = pl.BlockSpec(memory_space=pltpu.SMEM)
    hbm = pl.BlockSpec(memory_space=pl.ANY)
    hidden = pl.pallas_call(
        functools.partial(hidden_kernel, n_e=n_e, width=d_dev),
        in_specs=[smem, vmem, vmem, vmem, hbm, hbm],
        out_specs=vmem,
        out_shape=jax.ShapeDtypeStruct((n_e, 4 * n_tok, f_dev), jnp.bfloat16),
        scratch_shapes=[
            pltpu.VMEM((4 * n_tok, d_all), jnp.bfloat16),
            pltpu.VMEM((n_e, f_dev, d_all), jnp.bfloat16),
            pltpu.VMEM((n_e, f_dev, d_all), jnp.bfloat16),
            pltpu.SemaphoreType.DMA((2, n_e)),
        ],
        compiler_params=pltpu.CompilerParams(vmem_limit_bytes=44 << 20),
        name="hidden",
    )(at, mine, other, mix4, w_gate, w_up)

    zs = [swap(hidden, "tensor", k) for k in (2, 4, 6)]
    ys = [swap(b, "tensor", 1) for b in [hidden] + zs]
    own, away = pl.pallas_call(
        functools.partial(down_kernel, n_e=n_e, width=f_dev),
        in_specs=[smem] + [vmem] * 8 + [hbm],
        out_specs=[vmem, vmem],
        out_shape=[
            jax.ShapeDtypeStruct((n_tok, d_dev), jnp.float32),
            jax.ShapeDtypeStruct((3 * n_tok, d_dev), jnp.bfloat16),
        ],
        scratch_shapes=[
            pltpu.VMEM((n_e, 4 * n_tok, f_all), jnp.bfloat16),
            pltpu.VMEM((n_e, f_all, d_dev), jnp.bfloat16),
            pltpu.SemaphoreType.DMA((n_e,)),
        ],
        compiler_params=pltpu.CompilerParams(vmem_limit_bytes=40 << 20),
        name="down",
    )(at, hidden, *zs, *ys, w_down)
    total = own
    for j, k in enumerate(ROWS[1:]):
        total = total + swap(away[j * n_tok : (j + 1) * n_tok], "expert", k).astype(jnp.float32)
    return total.astype(jnp.bfloat16)


def on_device(*args):
    tokens, _, _, w_gate, _, _ = args
    n_e, n_t = lax.axis_size("expert"), lax.axis_size("tensor")
    fits = (n_e, n_t) == (4, 8) and n_e * tokens.shape[0] <= CAP
    tiled = tokens.shape[0] % 16 == 0 and tokens.shape[1] % 128 == 0 and w_gate.shape[1] % 128 == 0
    return planned(*args) if fits and tiled else general(*args)


def solution(mesh):
    placed = (
        P("expert", "tensor"),
        P("expert", None),
        P("expert", None),
        P("expert", "tensor", None),
        P("expert", "tensor", None),
        P("expert", None, "tensor"),
    )
    return jax.shard_map(
        on_device, mesh=mesh, in_specs=placed, out_specs=P("expert", "tensor"), check_vma=False
    )
```

```python
import functools

import jax
import jax.numpy as jnp
from jax import lax
from jax.experimental import pallas as pl
from jax.experimental.pallas import tpu as pltpu
from jax.sharding import PartitionSpec as P

CAP = 128


def entering(value, axis, combine, identity):
    length, index = (lax.axis_size(axis), lax.axis_index(axis))
    everything = lax.all_gather(value, axis)
    start = jnp.broadcast_to(jnp.asarray(identity, value.dtype), value.shape)

    def lap(k, before):
        reached = k < index
        new = combine(before, everything[k])
        return jnp.where(reached, new, before)

    return lax.fori_loop(0, length, lap, start)


def add_counts(earlier, later):
    return earlier + later


def general(tokens, routes, gates, w_gate, w_up, w_down):
    exp_dev = w_gate.shape[0]
    experts = exp_dev * lax.axis_size("expert")
    group_index = lax.axis_index("expert")
    expert_ids = jnp.arange(experts, dtype=jnp.int32)
    route_hits = routes[:, :, None] == expert_ids[None, None, :]
    member = jnp.sum(route_hits.astype(jnp.int32), axis=1)
    counts = jnp.sum(member, axis=0)
    offset = entering(counts, "expert", add_counts, jnp.zeros_like(counts))
    before = jnp.cumsum(member, axis=0) - member + offset[None, :]
    own_slot = jnp.sum(jnp.where(route_hits, before[:, None, :], 0), axis=2).astype(jnp.int32)
    all_routes, all_slots = (
        lax.all_gather(routes, "expert", axis=0, tiled=True),
        lax.all_gather(own_slot, "expert", axis=0, tiled=True),
    )
    row_block, all_gates = (
        lax.all_gather(tokens, "expert", axis=0, tiled=True),
        lax.all_gather(gates, "expert", axis=0, tiled=True),
    )
    gathered = lax.all_gather(row_block, "tensor", axis=1, tiled=True)
    local_ids = all_routes - group_index * exp_dev
    is_local = (local_ids >= 0) & (local_ids < exp_dev)
    slot_id = jnp.where(is_local, local_ids * CAP + all_slots, -1)
    slot_range = jnp.arange(exp_dev * CAP, dtype=jnp.int32)
    matches = slot_id[:, :, None] == slot_range[None, None, :]
    picked = jnp.any(matches, axis=1).astype(jnp.bfloat16)
    mixing = jnp.sum(jnp.where(matches, all_gates.astype(jnp.float32)[:, :, None], 0.0), axis=1)
    slot_rows = lax.dot_general(
        picked, gathered, (((0,), (0,)), ((), ())), preferred_element_type=jnp.float32
    ).astype(jnp.bfloat16)
    slot_rows = slot_rows.reshape(exp_dev, CAP, gathered.shape[1])
    gate_proj = jnp.einsum("ecd,efd->ecf", slot_rows, w_gate, preferred_element_type=jnp.float32)
    up_proj = jnp.einsum("ecd,efd->ecf", slot_rows, w_up, preferred_element_type=jnp.float32)
    hidden = (jax.nn.silu(gate_proj) * up_proj).astype(jnp.bfloat16)
    expert_out = jnp.einsum(
        "ecf,efd->ecd",
        lax.all_gather(hidden, "tensor", axis=2, tiled=True),
        w_down,
        preferred_element_type=jnp.float32,
    )
    expert_out = expert_out.reshape(exp_dev * CAP, w_down.shape[2])
    partial_value = jnp.dot(mixing, expert_out, precision=lax.Precision.HIGHEST)
    result = lax.psum_scatter(partial_value, "expert", scatter_dimension=0, tiled=True)
    return result.astype(jnp.bfloat16)


COLS = (0, 2, 4, 6, 1, 3, 5, 7)
ROWS = (0, 2, 1, 3)
CAPS = (192, 256, 320, 384)
EARLY = 5
NT = (((1,), (1,)), ((), ()))
VMEM = pl.BlockSpec(memory_space=pltpu.VMEM)
SMEM = pl.BlockSpec(memory_space=pltpu.SMEM)
HBM = pl.BlockSpec(memory_space=pltpu.HBM)


def swap(value, axis, k):
    n = lax.axis_size(axis)
    return lax.ppermute(value, axis, [(i, i ^ k) for i in range(n)])


def call(body, ins, outs, scratch, limit, *args):
    return pl.pallas_call(
        body,
        in_specs=ins,
        out_specs=[SMEM if d == jnp.int32 else VMEM for _, d in outs],
        out_shape=[jax.ShapeDtypeStruct(s, d) if d == jnp.int32 else pltpu.VMEM(s, d) for s, d in outs],
        scratch_shapes=scratch,
        compiler_params=pltpu.CompilerParams(vmem_limit_bytes=limit << 20),
    )(*(a if spec is SMEM else pltpu.with_memory_space_constraint(a, spec.memory_space) for spec, a in zip(ins, args)))


def column_copies(at, weights, bufs, sems, blocks, n_e, f_dev, width):
    made = []
    for b, (w, buf) in enumerate(zip(weights, bufs)):
        for e in range(n_e):
            for j, off in enumerate(blocks):
                col = pl.multiple_of((at[0] ^ off) * width, 128)
                src = w.at[e, :, pl.ds(col, width)]
                dst = buf.at[e * f_dev : (e + 1) * f_dev, j * width : (j + 1) * width]
                made.append(pltpu.make_async_copy(src, dst, sems.at[b, e, j]))
    return made


def pre_kernel(tokens, routes, gates, out, t_buf, r_buf, g_buf, sems, *, lanes):
    copies = [
        pltpu.make_async_copy(src, dst, sems.at[i])
        for i, (src, dst) in enumerate(((tokens, t_buf), (routes, r_buf), (gates, g_buf)))
    ]
    for c in copies:
        c.start()
    for c in copies:
        c.wait()
    d = tokens.shape[1]
    out[:, :d] = t_buf[...]
    ids = lax.broadcasted_iota(jnp.int32, (lanes, tokens.shape[0]), 0)
    mix = jnp.zeros(ids.shape, jnp.float32)
    picked, weights = r_buf[...], g_buf[...].astype(jnp.float32)
    for k in range(picked.shape[0]):
        mix = mix + jnp.where(picked[k : k + 1] == ids, weights[k : k + 1], 0.0)
    out[:, d:] = mix.T.astype(out.dtype)


def load_kernel(at, wg, wu, g_buf, u_buf, sems, *, n_e, f_dev, width):
    made = column_copies(at, (wg, wu), (g_buf, u_buf), sems, COLS[:EARLY], n_e, f_dev, width)
    for c in made:
        c.start()
    for c in made:
        c.wait()


def lay(x, mine, other, n, half, width):
    for j in range(n):
        x[:half, j * width : (j + 1) * width] = mine[j * half : (j + 1) * half, :]
        x[half:, j * width : (j + 1) * width] = other[j * half : (j + 1) * half, :]


def early_kernel(at, mine, other, g_in, u_in, wg, wu, g_acc, u_acc, mix_t, pos_t, pos_c, taken, g_buf, u_buf, x, m, sems, *, n_e, f_dev, width, half, caps):
    made = column_copies(at, (wg, wu), (g_buf, u_buf), sems, COLS[EARLY:], n_e, f_dev, width)
    for c in made:
        c.start()
    lay(x, mine, other, EARLY, half, width)

    def one(e, carry):
        rows = pl.ds(pl.multiple_of(e * f_dev, f_dev), f_dev)
        g_acc[rows, :] = lax.dot_general(g_in[rows, :], x[...], NT, preferred_element_type=jnp.float32)
        u_acc[rows, :] = lax.dot_general(u_in[rows, :], x[...], NT, preferred_element_type=jnp.float32)
        return carry

    lax.fori_loop(0, n_e, one, 0)
    lanes, rows = m.shape[0], 2 * half
    mix = jnp.concatenate([r[EARLY * half :, :lanes].astype(jnp.float32) for r in (mine, other)], axis=0)
    m[...] = mix.T
    own = m[pl.ds(at[1] * n_e, n_e), :]
    mix_t[...] = own
    member = own > 0.0
    ones = jnp.where(member, 1.0, 0.0)
    below = lax.broadcasted_iota(jnp.int32, (rows, rows), 0) < lax.broadcasted_iota(jnp.int32, (rows, rows), 1)
    rank = jnp.dot(ones.astype(jnp.bfloat16), jnp.where(below, 1.0, 0.0).astype(jnp.bfloat16), preferred_element_type=jnp.float32)
    start = jnp.zeros((1, 1), jnp.float32)
    m[...] = jnp.full(m.shape, -1.0, jnp.float32)
    for e in range(n_e):
        m[e : e + 1, :] = jnp.where(member[e : e + 1], rank[e : e + 1] + start, -1.0)
        start = start + jnp.sum(ones[e : e + 1], axis=1, keepdims=True)
    pos_t[...] = m[0:n_e, :]
    pos_c[...] = m[...].T
    total, case = start[0, 0], jnp.int32(0)
    for cap in caps:
        case = case + jnp.where(total > cap, 1, 0)
    taken[0] = case
    for c in made:
        c.wait()


def late_kernel(mine, other, g_in, u_in, g_acc, u_acc, mix_t, pos_t, packed, x, *, n_e, f_dev, width, half):
    lay(x, mine, other, len(COLS) - EARLY, half, width)
    slots = lax.broadcasted_iota(jnp.int32, (packed.shape[0], 2 * half), 0).astype(jnp.float32)
    acc = None
    for e in range(n_e):
        rows = slice(e * f_dev, (e + 1) * f_dev)
        g = g_acc[rows] + lax.dot_general(g_in[rows], x[...], NT, preferred_element_type=jnp.float32)
        u = u_acc[rows] + lax.dot_general(u_in[rows], x[...], NT, preferred_element_type=jnp.float32)
        h = (g / (1.0 + jnp.exp(-g)) * u * mix_t[e : e + 1, :]).astype(jnp.bfloat16)
        pick = jnp.where(slots == pos_t[e : e + 1, :], 1.0, 0.0).astype(jnp.bfloat16)
        part = lax.dot_general(pick, h, NT, preferred_element_type=jnp.float32)
        acc = part if acc is None else acc + part
    packed[...] = acc.astype(jnp.bfloat16)


def fetch_kernel(at, wd, d_buf, sems, *, n_e, f_dev):
    made = []
    for e in range(n_e):
        for j, off in enumerate(COLS):
            row = pl.multiple_of((at[0] ^ off) * f_dev, 128)
            dst = d_buf.at[e, j * f_dev : (j + 1) * f_dev, :]
            made.append(pltpu.make_async_copy(wd.at[e, pl.ds(row, f_dev), :], dst, sems.at[e, j]))
    for c in made:
        c.start()
    for c in made:
        c.wait()


def down(blocks, pos_c, wd, n_e, first):
    f_dev = blocks[0].shape[1]
    slots = lax.broadcasted_iota(jnp.int32, (pos_c.shape[0], blocks[0].shape[0]), 1).astype(jnp.float32)
    acc = None
    for e in range(n_e):
        place = jnp.where(slots == pos_c[:, e : e + 1], 1.0, 0.0).astype(jnp.bfloat16)
        h = [jnp.dot(place, b[...], preferred_element_type=jnp.float32).astype(jnp.bfloat16) for b in blocks]
        units = slice(first * f_dev, (first + len(blocks)) * f_dev)
        y = jnp.dot(jnp.concatenate(h, axis=1), wd[e, units, :], preferred_element_type=jnp.float32)
        acc = y if acc is None else acc + y
    return acc


def down_a_kernel(*refs, n_e):
    blocks, (pos_c, wd, acc) = refs[:EARLY], refs[EARLY:]
    acc[...] = down(blocks, pos_c, wd, n_e, 0)


def down_b_kernel(*refs, n_e):
    late = len(COLS) - EARLY
    blocks, (pos_c, wd, acc, own, away) = refs[:late], refs[late:]
    total = acc[...] + down(blocks, pos_c, wd, n_e, EARLY)
    n = own.shape[0]
    own[...] = total[:n]
    away[...] = total[n:].astype(jnp.bfloat16)


def planned(tokens, routes, gates, w_gate, w_up, w_down):
    n_tok, d_dev = tokens.shape
    n_e, f_dev, _ = w_gate.shape
    f_all = w_down.shape[1]
    half, rows, n = 2 * n_tok, 4 * n_tok, len(COLS)
    bf16, f32, dma = jnp.bfloat16, jnp.float32, pltpu.SemaphoreType.DMA
    at = jnp.stack([lax.axis_index("tensor"), lax.axis_index("expert")]).astype(jnp.int32)
    sizes = dict(n_e=n_e, f_dev=f_dev, width=d_dev)

    (first,) = call(functools.partial(pre_kernel, lanes=128), [HBM] * 3, [((n_tok, d_dev + 128), bf16)],
        [pltpu.VMEM(tokens.shape, bf16), pltpu.VMEM(routes.T.shape, jnp.int32), pltpu.VMEM(gates.T.shape, bf16), dma((3,))],
        4, tokens, routes.T, gates.T,
    )
    second = swap(first, "expert", 2)
    both = jnp.concatenate([first, second], axis=0)
    block, mix2 = both[:, :d_dev], both[:, d_dev:]
    wide = [((n_e * f_dev, EARLY * d_dev), bf16)] * 2
    g_a, u_a = call(
        functools.partial(load_kernel, **sizes), [SMEM, HBM, HBM], wide, [dma((2, n_e, EARLY))], 4, at, w_gate, w_up
    )
    y1 = swap(block, "tensor", 1)
    z2, z4, z6 = (swap(block, "tensor", k) for k in (2, 4, 6))
    y3, y5, y7 = (swap(z, "tensor", 1) for z in (z2, z4, z6))
    mix2 = jnp.pad(mix2, ((0, 0), (0, d_dev - 128)))
    mine_a = jnp.concatenate([block, z2, z4, z6, y1, mix2], axis=0)
    other_a = swap(mine_a, "expert", 1)
    late = n - EARLY
    caps = [c for c in CAPS if c < n_e * rows] + [n_e * rows]
    g_acc, u_acc, mix_t, pos_t, pos_c, taken, g_b, u_b = call(
        functools.partial(early_kernel, half=half, caps=caps[:-1], **sizes),
        [SMEM, VMEM, VMEM, VMEM, VMEM, HBM, HBM],
        [((n_e * f_dev, rows), f32)] * 2
        + [((n_e, rows), f32)] * 2
        + [((rows, 128), f32), ((1,), jnp.int32)]
        + [((n_e * f_dev, late * d_dev), bf16)] * 2,
        [pltpu.VMEM((rows, EARLY * d_dev), bf16), pltpu.VMEM((128, rows), f32), dma((2, n_e, late))],
        8,
        at, mine_a, other_a, g_a, u_a, w_gate, w_up,
    )
    mine_b = jnp.concatenate([y3, y5, y7], axis=0)
    other_b = swap(mine_b, "expert", 1)
    (packed,) = call(
        functools.partial(late_kernel, half=half, **sizes),
        [VMEM] * 8,
        [((n_e * rows, f_dev), bf16)],
        [pltpu.VMEM((rows, late * d_dev), bf16)],
        8,
        mine_b, other_b, g_b, u_b, g_acc, u_acc, mix_t, pos_t,
    )

    def finish(cap, packed, pos_c, w_down, at):
        hidden = packed[:cap]
        (wd,) = call(
            functools.partial(fetch_kernel, n_e=n_e, f_dev=f_dev), [SMEM, HBM], [((n_e, f_all, d_dev), bf16)], [dma((n_e, n))], 4, at, w_down
        )
        h1 = swap(hidden, "tensor", 1)
        h2, h4, h6 = (swap(hidden, "tensor", k) for k in (2, 4, 6))
        h3, h5, h7 = (swap(h, "tensor", 1) for h in (h2, h4, h6))
        (acc,) = call(
            functools.partial(down_a_kernel, n_e=n_e), [VMEM] * (EARLY + 2), [((rows, d_dev), f32)], [], 16,
            hidden, h2, h4, h6, h1, pos_c, wd,
        )
        return call(
            functools.partial(down_b_kernel, n_e=n_e), [VMEM] * (late + 3),
            [((n_tok, d_dev), f32), ((3 * n_tok, d_dev), bf16)], [], 16,
            h3, h5, h7, pos_c, wd, acc,
        )

    own, away = lax.switch(taken[0], [functools.partial(finish, c) for c in caps], packed, pos_c, w_down, at)
    total = own
    for j, k in enumerate(ROWS[1:]):
        piece = swap(away[j * n_tok : (j + 1) * n_tok], "expert", k)
        total = total + piece.astype(f32)
    return total.astype(bf16)


def on_device(*args):
    tokens, _, _, w_gate, _, _ = args
    n_e, n_t = lax.axis_size("expert"), lax.axis_size("tensor")
    fits = (n_e, n_t) == (4, 8) and n_e * tokens.shape[0] == CAP
    tiled = tokens.shape[0] % 16 == 0 and tokens.shape[1] % 128 == 0 and w_gate.shape[1] % 128 == 0
    if not (fits and tiled):
        return general(*args)
    return planned(*args)


def solution(mesh):
    placed = (
        P("expert", "tensor"),
        P("expert", None),
        P("expert", None),
        P("expert", "tensor", None),
        P("expert", "tensor", None),
        P("expert", None, "tensor"),
    )
    return jax.shard_map(
        on_device, mesh=mesh, in_specs=placed, out_specs=P("expert", "tensor"), check_vma=False
    )
```

```python
import functools

import jax
import jax.numpy as jnp
from jax import lax
from jax.experimental import pallas as pl
from jax.experimental.pallas import tpu as pltpu
from jax.sharding import PartitionSpec as P

CAP = 128


def entering(value, axis, combine, identity):
    length, index = (lax.axis_size(axis), lax.axis_index(axis))
    everything = lax.all_gather(value, axis)
    start = jnp.broadcast_to(jnp.asarray(identity, value.dtype), value.shape)

    def lap(k, before):
        reached = k < index
        new = combine(before, everything[k])
        return jnp.where(reached, new, before)

    return lax.fori_loop(0, length, lap, start)


def add_counts(earlier, later):
    return earlier + later


def general(tokens, routes, gates, w_gate, w_up, w_down):
    exp_dev = w_gate.shape[0]
    experts = exp_dev * lax.axis_size("expert")
    group_index = lax.axis_index("expert")
    expert_ids = jnp.arange(experts, dtype=jnp.int32)
    route_hits = routes[:, :, None] == expert_ids[None, None, :]
    member = jnp.sum(route_hits.astype(jnp.int32), axis=1)
    counts = jnp.sum(member, axis=0)
    offset = entering(counts, "expert", add_counts, jnp.zeros_like(counts))
    before = jnp.cumsum(member, axis=0) - member + offset[None, :]
    own_slot = jnp.sum(jnp.where(route_hits, before[:, None, :], 0), axis=2).astype(jnp.int32)
    all_routes, all_slots = (
        lax.all_gather(routes, "expert", axis=0, tiled=True),
        lax.all_gather(own_slot, "expert", axis=0, tiled=True),
    )
    row_block, all_gates = (
        lax.all_gather(tokens, "expert", axis=0, tiled=True),
        lax.all_gather(gates, "expert", axis=0, tiled=True),
    )
    gathered = lax.all_gather(row_block, "tensor", axis=1, tiled=True)
    local_ids = all_routes - group_index * exp_dev
    is_local = (local_ids >= 0) & (local_ids < exp_dev)
    slot_id = jnp.where(is_local, local_ids * CAP + all_slots, -1)
    slot_range = jnp.arange(exp_dev * CAP, dtype=jnp.int32)
    matches = slot_id[:, :, None] == slot_range[None, None, :]
    picked = jnp.any(matches, axis=1).astype(jnp.bfloat16)
    mixing = jnp.sum(jnp.where(matches, all_gates.astype(jnp.float32)[:, :, None], 0.0), axis=1)
    slot_rows = lax.dot_general(
        picked, gathered, (((0,), (0,)), ((), ())), preferred_element_type=jnp.float32
    ).astype(jnp.bfloat16)
    slot_rows = slot_rows.reshape(exp_dev, CAP, gathered.shape[1])
    gate_proj = jnp.einsum("ecd,efd->ecf", slot_rows, w_gate, preferred_element_type=jnp.float32)
    up_proj = jnp.einsum("ecd,efd->ecf", slot_rows, w_up, preferred_element_type=jnp.float32)
    hidden = (jax.nn.silu(gate_proj) * up_proj).astype(jnp.bfloat16)
    expert_out = jnp.einsum(
        "ecf,efd->ecd",
        lax.all_gather(hidden, "tensor", axis=2, tiled=True),
        w_down,
        preferred_element_type=jnp.float32,
    )
    expert_out = expert_out.reshape(exp_dev * CAP, w_down.shape[2])
    partial_value = jnp.dot(mixing, expert_out, precision=lax.Precision.HIGHEST)
    result = lax.psum_scatter(partial_value, "expert", scatter_dimension=0, tiled=True)
    return result.astype(jnp.bfloat16)


COLS = (0, 1, 2, 4, 3, 5, 6, 7)
HERE, BESIDE = (0, 2, 4, 6), (1, 3, 5, 7)
ROWS = (0, 2, 1, 3)
CAPS = (192, 224, 256, 288, 320, 352, 384)
EARLY = 6
NT = (((1,), (1,)), ((), ()))
VMEM = pl.BlockSpec(memory_space=pltpu.VMEM)
SMEM = pl.BlockSpec(memory_space=pltpu.SMEM)
HBM = pl.BlockSpec(memory_space=pltpu.HBM)


def swap(value, axis, k):
    n = lax.axis_size(axis)
    return lax.ppermute(value, axis, [(i, i ^ k) for i in range(n)])


def call(body, ins, outs, scratch, limit, *args):
    return pl.pallas_call(
        body,
        in_specs=ins,
        out_specs=[SMEM if d == jnp.int32 else VMEM for _, d in outs],
        out_shape=[pltpu.SMEM(s, d) if d == jnp.int32 else pltpu.VMEM(s, d) for s, d in outs],
        scratch_shapes=scratch,
        compiler_params=pltpu.CompilerParams(vmem_limit_bytes=limit << 20),
    )(*(a if spec is SMEM else pltpu.with_memory_space_constraint(a, spec.memory_space) for spec, a in zip(ins, args)))


class Columns:
    def __init__(self, at, w, buf, sems, experts, blocks, width):
        self.at, self.w, self.buf, self.sems = at, w, buf, sems
        self.first, self.count, self.blocks, self.width = experts[0], experts[1] - experts[0], blocks, width

    def copy(self, i, j):
        f_dev, width = self.w.shape[1], self.width
        col = pl.multiple_of((self.at[0] ^ self.blocks[j]) * width, 128)
        rows = pl.ds(pl.multiple_of(i * f_dev, f_dev), f_dev)
        dst = self.buf.at[rows, j * width : (j + 1) * width]
        return pltpu.make_async_copy(self.w.at[self.first + i, :, pl.ds(col, width)], dst, self.sems.at[i, j])

    def start(self):
        def one(i, carry):
            for j in range(len(self.blocks)):
                self.copy(i, j).start()
            return carry

        lax.fori_loop(0, self.count, one, 0)

    def wait(self):
        def one(i, carry):
            for j in range(len(self.blocks)):
                self.copy(i, j).wait()
            return carry

        lax.fori_loop(0, self.count, one, 0)


def pre_kernel(tokens, routes, gates, tok, mix, r_buf, g_buf, sems):
    copies = [
        pltpu.make_async_copy(src, dst, sems.at[i])
        for i, (src, dst) in enumerate(((tokens, tok), (routes, r_buf), (gates, g_buf)))
    ]
    for c in copies:
        c.start()
    for c in copies:
        c.wait()
    picked, weights = r_buf[...], g_buf[...].astype(jnp.float32)
    n = picked.shape[1]
    ids = lax.broadcasted_iota(jnp.int32, (mix.shape[0], n), 0)
    total = jnp.zeros(ids.shape, jnp.float32)
    for k in range(picked.shape[0]):
        total = total + jnp.where(picked[k : k + 1] == ids, weights[k : k + 1], 0.0)
    mix[...] = jnp.zeros(mix.shape, mix.dtype)
    mix[:, :n] = total.astype(mix.dtype)


def load_kernel(at, wg, wu, *refs, jobs, width):
    bufs, sems = refs[: len(jobs)], refs[len(jobs) :]
    made = [
        Columns(at, (wg, wu)[which], buf, sem, experts, blocks, width)
        for (which, experts, blocks), buf, sem in zip(jobs, bufs, sems)
    ]
    for c in made:
        c.start()
    for c in made:
        c.wait()


def lay(x, mine, other, n_tok, width, second):
    for r, src in enumerate((mine, mine, other, other)):
        for j in range(len(HERE)):
            at = r % 2 * second + j * n_tok
            x[r * n_tok : (r + 1) * n_tok, j * width : (j + 1) * width] = src[at : at + n_tok, :]


def product(acc, pieces, x):
    base = 0
    for w in pieces:
        acc[base : base + w.shape[0], :] = lax.dot_general(w[...], x[...], NT, preferred_element_type=jnp.float32)
        base += w.shape[0]


def early_g_kernel(at, mine, other, g_in, wg, x, g_acc, mix_t, pos_t, pos_c, taken, g_buf, m, sems, *, n_e, f_dev, n_tok, width, caps):
    made = Columns(at, wg, g_buf, sems, (n_e // 2, n_e), BESIDE, width)
    made.start()
    lay(x, mine, other, n_tok, width, mine.shape[0] // 2)
    product(g_acc, [g_in], x)
    rows, lanes, block = 4 * n_tok, m.shape[1], mine.shape[0] // 2
    mix = None
    for r, src in enumerate((mine, mine, other, other)):
        lo = r % 2 * block + len(HERE) * n_tok
        part = src[lo : (r % 2 + 1) * block, :lanes].astype(jnp.float32)
        part = pltpu.roll(part, r * n_tok, 1) if r else part
        mix = part if mix is None else mix + part
    m[: mix.shape[0], :] = mix
    own = m[pl.ds(at[1] * n_e, n_e), :]
    mix_t[...] = own
    member = own > 0.0
    ones = jnp.where(member, 1.0, 0.0)
    below = lax.broadcasted_iota(jnp.int32, (rows, rows), 0) < lax.broadcasted_iota(jnp.int32, (rows, rows), 1)
    below = jnp.where(below, 1.0, 0.0).astype(jnp.bfloat16)
    rank = jnp.dot(ones.astype(jnp.bfloat16), below, preferred_element_type=jnp.float32)
    start = jnp.zeros((1, 1), jnp.float32)
    m[...] = jnp.full(m.shape, -1.0, jnp.float32)
    for e in range(n_e):
        m[e : e + 1, :] = jnp.where(member[e : e + 1], rank[e : e + 1] + start, -1.0)
        start = start + jnp.sum(ones[e : e + 1], axis=1, keepdims=True)
    pos_t[...] = m[0:n_e, :]
    columns = m[...].T
    for e in range(n_e):
        pos_c[e * rows : (e + 1) * rows, :] = jnp.broadcast_to(columns[:, e : e + 1], (rows, pos_c.shape[1]))
    total, case = start[0, 0], jnp.int32(0)
    for cap in caps:
        case = case + jnp.where(total > cap, 1, 0)
    taken[0] = case
    made.wait()


def early_u_kernel(at, x, u_in0, u_in1, wu, u_acc, u_buf, sems, *, n_e, f_dev, width):
    made = Columns(at, wu, u_buf, sems, (0, n_e // 2), BESIDE, width)
    made.start()
    product(u_acc, [u_in0, u_in1], x)
    made.wait()


def late_kernel(at, mine, other, g_in0, g_in1, u_in0, wu, g_acc, u_acc, mix_t, pos_t, packed, x, u_in1, sems, *, n_e, f_dev, n_tok, width):
    made = Columns(at, wu, u_in1, sems, (n_e // 2, n_e), BESIDE, width)
    made.start()
    lay(x, mine, other, n_tok, width, mine.shape[0] // 2)
    slots = lax.broadcasted_iota(jnp.int32, (packed.shape[0], 4 * n_tok), 0).astype(jnp.float32)
    acc = None
    for e in range(n_e):
        side, i = divmod(e, n_e // 2)
        here = slice(i * f_dev, (i + 1) * f_dev)
        rows = slice(e * f_dev, (e + 1) * f_dev)
        g = g_acc[rows] + lax.dot_general((g_in0, g_in1)[side][here], x[...], NT, preferred_element_type=jnp.float32)
        if e == n_e // 2:
            made.wait()
        u = u_acc[rows] + lax.dot_general((u_in0, u_in1)[side][here], x[...], NT, preferred_element_type=jnp.float32)
        h = (g / (1.0 + jnp.exp(-g)) * u * mix_t[e : e + 1, :]).astype(jnp.bfloat16)
        pick = jnp.where(slots == pos_t[e : e + 1, :], 1.0, 0.0).astype(jnp.bfloat16)
        part = lax.dot_general(pick, h, NT, preferred_element_type=jnp.float32)
        acc = part if acc is None else acc + part
    packed[...] = acc.astype(jnp.bfloat16)


def fetch_kernel(at, wd, d_buf, sems, *, n_e, f_dev):
    made = []
    for e in range(n_e):
        for j, off in enumerate(COLS):
            row = pl.multiple_of((at[0] ^ off) * f_dev, 128)
            dst = d_buf.at[e, j * f_dev : (j + 1) * f_dev, :]
            made.append(pltpu.make_async_copy(wd.at[e, pl.ds(row, f_dev), :], dst, sems.at[e, j]))
    for c in made:
        c.start()
    for c in made:
        c.wait()


def down(acc, blocks, pos, wd, first, unroll):
    cap, f_dev = blocks[0].shape
    rows, lanes = acc.shape[0], pos.shape[1]
    slots = lax.broadcasted_iota(jnp.int32, (rows, lanes), 1).astype(jnp.float32)

    def one(e, carry):
        here = pos[pl.ds(pl.multiple_of(e * rows, rows), rows), :]
        place = [jnp.where(slots + float(lo) == here, 1.0, 0.0) for lo in range(0, cap, lanes)]
        place = jnp.concatenate(place, axis=1)[:, :cap].astype(jnp.bfloat16)
        h = [jnp.dot(place, b[...], preferred_element_type=jnp.float32).astype(jnp.bfloat16) for b in blocks]
        units = slice(first * f_dev, (first + len(blocks)) * f_dev)
        acc[...] += jnp.dot(jnp.concatenate(h, axis=1), wd[e, units, :], preferred_element_type=jnp.float32)
        return carry

    lax.fori_loop(0, wd.shape[0], one, 0, unroll=unroll)


def down_a_kernel(*refs):
    blocks, (pos, wd, acc) = refs[:EARLY], refs[EARLY:]
    acc[...] = jnp.zeros(acc.shape, acc.dtype)
    down(acc, blocks, pos, wd, 0, 1)


def down_b_kernel(*refs):
    late = len(COLS) - EARLY
    blocks, (pos, wd, acc, out) = refs[:late], refs[late:]
    out[...] = acc[...]
    down(out, blocks, pos, wd, EARLY, 2)


def planned(tokens, routes, gates, w_gate, w_up, w_down):
    n_tok, d_dev = tokens.shape
    n_e, f_dev, _ = w_gate.shape
    f_all = w_down.shape[1]
    rows, n = 4 * n_tok, len(COLS)
    experts = n_e * lax.axis_size("expert")
    bf16, f32, dma = jnp.bfloat16, jnp.float32, pltpu.SemaphoreType.DMA
    at = jnp.stack([lax.axis_index("tensor"), lax.axis_index("expert")]).astype(jnp.int32)
    sizes = dict(n_e=n_e, f_dev=f_dev, width=d_dev)
    mid, k_half = n_e // 2, len(HERE) * d_dev
    whole, part = ((n_e * f_dev, k_half), bf16), ((mid * f_dev, k_half), bf16)
    whole_sems, part_sems = dma((n_e, len(HERE))), dma((mid, len(HERE)))
    sums = ((n_e * f_dev, rows), f32)
    half = pltpu.VMEM((rows, len(HERE) * d_dev), bf16)
    caps = [c for c in CAPS if c < n_e * rows] + [n_e * rows]

    tok, mix = call(
        pre_kernel, [HBM] * 3, [((n_tok, d_dev), bf16), ((experts, d_dev), bf16)],
        [pltpu.VMEM(routes.T.shape, jnp.int32), pltpu.VMEM(gates.T.shape, bf16), dma((3,))],
        4, tokens, routes.T, gates.T,
    )
    z2, z4, z6 = (swap(tok, "tensor", k) for k in (2, 4, 6))

    def load(jobs):
        shapes = [whole if hi - lo == n_e else part for _, (lo, hi), _ in jobs]
        sems = [whole_sems if hi - lo == n_e else part_sems for _, (lo, hi), _ in jobs]
        body = functools.partial(load_kernel, jobs=jobs, width=d_dev)
        return call(body, [SMEM, HBM, HBM], shapes, sems, 4, at, w_gate, w_up)

    g_a, u_a0 = load(((0, (0, n_e), HERE), (1, (0, mid), HERE)))
    line = jnp.concatenate([tok, z2, z4, z6, mix], axis=0)
    line_x = swap(line, "expert", 2)
    line_y = swap(line[:rows], "tensor", 1)
    u_a1, g_b0 = load(((1, (mid, n_e), HERE), (0, (0, mid), BESIDE)))
    side_1 = swap(line_x[: rows // 2], "tensor", 1)
    side_2 = swap(line_y[rows // 2 :], "expert", 2)
    mine_a = jnp.concatenate([line, line_x], axis=0)
    other_a = swap(mine_a, "expert", 1)
    x_a, g_acc, mix_t, pos_t, pos_c, taken, g_b1 = call(
        functools.partial(early_g_kernel, n_tok=n_tok, caps=caps[:-1], **sizes),
        [SMEM, VMEM, VMEM, VMEM, HBM],
        [(half.shape, bf16), sums, ((n_e, rows), f32), ((n_e, rows), f32), ((n_e * rows, 128), f32), ((1,), jnp.int32), part],
        [pltpu.VMEM((128, rows), f32), part_sems],
        8, at, mine_a, other_a, g_a, w_gate,
    )
    mine_b = jnp.concatenate([line_y, side_1, side_2], axis=0)
    other_b = swap(mine_b, "expert", 1)
    u_acc, u_b0 = call(
        functools.partial(early_u_kernel, **sizes),
        [SMEM, VMEM, VMEM, VMEM, HBM], [sums, part], [part_sems], 8, at, x_a, u_a0, u_a1, w_up,
    )
    (packed,) = call(
        functools.partial(late_kernel, n_tok=n_tok, **sizes),
        [SMEM] + [VMEM] * 5 + [HBM] + [VMEM] * 4, [((n_e * rows, f_dev), bf16)],
        [half, pltpu.VMEM(part[0], bf16), part_sems], 12,
        at, mine_b, other_b, g_b0, g_b1, u_b0, w_up, g_acc, u_acc, mix_t, pos_t,
    )

    def finish(cap, packed, pos_c, w_down, at):
        hidden = packed[:cap]
        (wd,) = call(
            functools.partial(fetch_kernel, n_e=n_e, f_dev=f_dev), [SMEM, HBM], [((n_e, f_all, d_dev), bf16)], [dma((n_e, n))], 4, at, w_down
        )
        h1 = swap(hidden, "tensor", 1)
        h2, h4 = (swap(hidden, "tensor", k) for k in (2, 4))
        h3, h5 = (swap(h, "tensor", 1) for h in (h2, h4))
        h6, h7 = (swap(h, "tensor", 2) for h in (h4, h5))
        (acc,) = call(
            down_a_kernel, [VMEM] * (EARLY + 2), [((rows, d_dev), f32)], [], 16,
            hidden, h1, h2, h4, h3, h5, pos_c, wd,
        )
        return call(
            down_b_kernel, [VMEM] * (n - EARLY + 3),
            [((rows, d_dev), f32)], [], 16,
            h6, h7, pos_c, wd, acc,
        )[0]

    summed = lax.switch(taken[0], [functools.partial(finish, c) for c in caps], packed, pos_c, w_down, at)
    total = summed[:n_tok]
    for j, k in enumerate(ROWS[1:], 1):
        piece = swap(summed[j * n_tok : (j + 1) * n_tok].astype(bf16), "expert", k)
        total = total + piece.astype(f32)
    return total.astype(bf16)


def on_device(*args):
    tokens, _, _, w_gate, _, _ = args
    n_e, n_t = lax.axis_size("expert"), lax.axis_size("tensor")
    fits = (n_e, n_t) == (4, 8) and n_e * tokens.shape[0] == CAP
    tiled = w_gate.shape[0] % 2 == 0 and tokens.shape[0] % 16 == 0 and tokens.shape[1] % 128 == 0 and w_gate.shape[1] % 128 == 0
    if not (fits and tiled):
        return general(*args)
    return planned(*args)


def solution(mesh):
    placed = (
        P("expert", "tensor"),
        P("expert", None),
        P("expert", None),
        P("expert", "tensor", None),
        P("expert", "tensor", None),
        P("expert", None, "tensor"),
    )
    return jax.shard_map(
        on_device, mesh=mesh, in_specs=placed, out_specs=P("expert", "tensor"), check_vma=False
    )
```

```python
import functools

import jax
import jax.numpy as jnp
from jax import lax
from jax.experimental import pallas as pl
from jax.experimental.pallas import tpu as pltpu
from jax.sharding import PartitionSpec as P

CAP = 128


def entering(value, axis, combine, identity):
    length, index = (lax.axis_size(axis), lax.axis_index(axis))
    everything = lax.all_gather(value, axis)
    start = jnp.broadcast_to(jnp.asarray(identity, value.dtype), value.shape)

    def lap(k, before):
        reached = k < index
        new = combine(before, everything[k])
        return jnp.where(reached, new, before)

    return lax.fori_loop(0, length, lap, start)


def add_counts(earlier, later):
    return earlier + later


def general(tokens, routes, gates, w_gate, w_up, w_down):
    exp_dev = w_gate.shape[0]
    experts = exp_dev * lax.axis_size("expert")
    group_index = lax.axis_index("expert")
    expert_ids = jnp.arange(experts, dtype=jnp.int32)
    route_hits = routes[:, :, None] == expert_ids[None, None, :]
    member = jnp.sum(route_hits.astype(jnp.int32), axis=1)
    counts = jnp.sum(member, axis=0)
    offset = entering(counts, "expert", add_counts, jnp.zeros_like(counts))
    before = jnp.cumsum(member, axis=0) - member + offset[None, :]
    own_slot = jnp.sum(jnp.where(route_hits, before[:, None, :], 0), axis=2).astype(jnp.int32)
    all_routes, all_slots = (
        lax.all_gather(routes, "expert", axis=0, tiled=True),
        lax.all_gather(own_slot, "expert", axis=0, tiled=True),
    )
    row_block, all_gates = (
        lax.all_gather(tokens, "expert", axis=0, tiled=True),
        lax.all_gather(gates, "expert", axis=0, tiled=True),
    )
    gathered = lax.all_gather(row_block, "tensor", axis=1, tiled=True)
    local_ids = all_routes - group_index * exp_dev
    is_local = (local_ids >= 0) & (local_ids < exp_dev)
    slot_id = jnp.where(is_local, local_ids * CAP + all_slots, -1)
    slot_range = jnp.arange(exp_dev * CAP, dtype=jnp.int32)
    matches = slot_id[:, :, None] == slot_range[None, None, :]
    picked = jnp.any(matches, axis=1).astype(jnp.bfloat16)
    mixing = jnp.sum(jnp.where(matches, all_gates.astype(jnp.float32)[:, :, None], 0.0), axis=1)
    slot_rows = lax.dot_general(
        picked, gathered, (((0,), (0,)), ((), ())), preferred_element_type=jnp.float32
    ).astype(jnp.bfloat16)
    slot_rows = slot_rows.reshape(exp_dev, CAP, gathered.shape[1])
    gate_proj = jnp.einsum("ecd,efd->ecf", slot_rows, w_gate, preferred_element_type=jnp.float32)
    up_proj = jnp.einsum("ecd,efd->ecf", slot_rows, w_up, preferred_element_type=jnp.float32)
    hidden = (jax.nn.silu(gate_proj) * up_proj).astype(jnp.bfloat16)
    expert_out = jnp.einsum(
        "ecf,efd->ecd",
        lax.all_gather(hidden, "tensor", axis=2, tiled=True),
        w_down,
        preferred_element_type=jnp.float32,
    )
    expert_out = expert_out.reshape(exp_dev * CAP, w_down.shape[2])
    partial_value = jnp.dot(mixing, expert_out, precision=lax.Precision.HIGHEST)
    result = lax.psum_scatter(partial_value, "expert", scatter_dimension=0, tiled=True)
    return result.astype(jnp.bfloat16)


COLS = (0, 1, 2, 4, 3, 5, 6, 7)
HERE, BESIDE = (0, 2, 4, 6), (1, 3, 5, 7)
ROWS = (0, 2, 1, 3)
CAPS = (192, 224, 256, 288, 304, 320, 336, 352, 384)
EARLY = 6
NT = (((1,), (1,)), ((), ()))
VMEM = pl.BlockSpec(memory_space=pltpu.VMEM)
SMEM = pl.BlockSpec(memory_space=pltpu.SMEM)
HBM = pl.BlockSpec(memory_space=pltpu.HBM)


def swap(value, axis, k):
    n = lax.axis_size(axis)
    return lax.ppermute(value, axis, [(i, i ^ k) for i in range(n)])


def call(body, ins, outs, scratch, limit, *args):
    return pl.pallas_call(
        body,
        in_specs=ins,
        out_specs=[SMEM if d == jnp.int32 else VMEM for _, d in outs],
        out_shape=[pltpu.SMEM(s, d) if d == jnp.int32 else pltpu.VMEM(s, d) for s, d in outs],
        scratch_shapes=scratch,
        compiler_params=pltpu.CompilerParams(vmem_limit_bytes=limit << 20),
    )(*(a if spec is SMEM else pltpu.with_memory_space_constraint(a, spec.memory_space) for spec, a in zip(ins, args)))


class Columns:
    def __init__(self, at, w, buf, sems, experts, blocks, width):
        self.at, self.w, self.buf, self.sems = at, w, buf, sems
        self.first, self.count, self.blocks, self.width = experts[0], experts[1] - experts[0], blocks, width

    def copy(self, i, j):
        f_dev, width = self.w.shape[1], self.width
        col = pl.multiple_of((self.at[0] ^ self.blocks[j]) * width, 128)
        rows = pl.ds(pl.multiple_of(i * f_dev, f_dev), f_dev)
        dst = self.buf.at[rows, j * width : (j + 1) * width]
        return pltpu.make_async_copy(self.w.at[self.first + i, :, pl.ds(col, width)], dst, self.sems.at[i, j])

    def start(self):
        def one(i, carry):
            for j in range(len(self.blocks)):
                self.copy(i, j).start()
            return carry

        lax.fori_loop(0, self.count, one, 0)

    def wait(self):
        def one(i, carry):
            for j in range(len(self.blocks)):
                self.copy(i, j).wait()
            return carry

        lax.fori_loop(0, self.count, one, 0)


def pre_kernel(tokens, routes, gates, tok, mix, r_buf, g_buf, sems):
    copies = [
        pltpu.make_async_copy(src, dst, sems.at[i])
        for i, (src, dst) in enumerate(((tokens, tok), (routes, r_buf), (gates, g_buf)))
    ]
    for c in copies:
        c.start()
    for c in copies:
        c.wait()
    picked, weights = r_buf[...], g_buf[...].astype(jnp.float32)
    n = picked.shape[1]
    ids = lax.broadcasted_iota(jnp.int32, (mix.shape[0], n), 0)
    total = jnp.zeros(ids.shape, jnp.float32)
    for k in range(picked.shape[0]):
        total = total + jnp.where(picked[k : k + 1] == ids, weights[k : k + 1], 0.0)
    mix[...] = jnp.zeros(mix.shape, mix.dtype)
    mix[:, :n] = total.astype(mix.dtype)


def load_kernel(at, wg, wu, *refs, jobs, width):
    bufs, sems = refs[: len(jobs)], refs[len(jobs) :]
    made = [
        Columns(at, (wg, wu)[which], buf, sem, experts, blocks, width)
        for (which, experts, blocks), buf, sem in zip(jobs, bufs, sems)
    ]
    for c in made:
        c.start()
    for c in made:
        c.wait()


def lay(x, mine, other, n_tok, width, second):
    for r, src in enumerate((mine, mine, other, other)):
        for j in range(len(HERE)):
            at = r % 2 * second + j * n_tok
            x[r * n_tok : (r + 1) * n_tok, j * width : (j + 1) * width] = src[at : at + n_tok, :]


def product(acc, pieces, x):
    base = 0
    for w in pieces:
        acc[base : base + w.shape[0], :] = lax.dot_general(w[...], x[...], NT, preferred_element_type=jnp.float32)
        base += w.shape[0]


def early_g_kernel(at, mine, other, g_in, wg, x, g_acc, mix_t, pos_t, pos_c, taken, g_buf, m, sems, *, n_e, f_dev, n_tok, width, caps):
    made = Columns(at, wg, g_buf, sems, (n_e // 2, n_e), BESIDE, width)
    made.start()
    lay(x, mine, other, n_tok, width, mine.shape[0] // 2)
    product(g_acc, [g_in], x)
    rows, lanes, block = 4 * n_tok, m.shape[1], mine.shape[0] // 2
    mix = None
    for r, src in enumerate((mine, mine, other, other)):
        lo = r % 2 * block + len(HERE) * n_tok
        part = src[lo : (r % 2 + 1) * block, :lanes].astype(jnp.float32)
        part = pltpu.roll(part, r * n_tok, 1) if r else part
        mix = part if mix is None else mix + part
    m[: mix.shape[0], :] = mix
    own = m[pl.ds(at[1] * n_e, n_e), :]
    mix_t[...] = own
    member = own > 0.0
    ones = jnp.where(member, 1.0, 0.0)
    below = lax.broadcasted_iota(jnp.int32, (rows, rows), 0) < lax.broadcasted_iota(jnp.int32, (rows, rows), 1)
    below = jnp.where(below, 1.0, 0.0).astype(jnp.bfloat16)
    rank = jnp.dot(ones.astype(jnp.bfloat16), below, preferred_element_type=jnp.float32)
    start = jnp.zeros((1, 1), jnp.float32)
    m[...] = jnp.full(m.shape, -1.0, jnp.float32)
    for e in range(n_e):
        m[e : e + 1, :] = jnp.where(member[e : e + 1], rank[e : e + 1] + start, -1.0)
        start = start + jnp.sum(ones[e : e + 1], axis=1, keepdims=True)
    pos_t[...] = m[0:n_e, :]
    columns = m[...].T
    for e in range(n_e):
        pos_c[e * rows : (e + 1) * rows, :] = jnp.broadcast_to(columns[:, e : e + 1], (rows, pos_c.shape[1]))
    total, case = start[0, 0], jnp.int32(0)
    for cap in caps:
        case = case + jnp.where(total > cap, 1, 0)
    taken[0] = case
    made.wait()


def early_u_kernel(at, x, u_in0, u_in1, wu, u_acc, u_buf, sems, *, n_e, f_dev, width):
    made = Columns(at, wu, u_buf, sems, (0, n_e // 2), BESIDE, width)
    made.start()
    product(u_acc, [u_in0, u_in1], x)
    made.wait()


def late_kernel(at, mine, other, g_in0, g_in1, u_in0, wu, g_acc, u_acc, mix_t, pos_t, packed, x, u_in1, sems, *, n_e, f_dev, n_tok, width):
    made = Columns(at, wu, u_in1, sems, (n_e // 2, n_e), BESIDE, width)
    made.start()
    lay(x, mine, other, n_tok, width, mine.shape[0] // 2)
    slots = lax.broadcasted_iota(jnp.int32, (packed.shape[0], 4 * n_tok), 0).astype(jnp.float32)
    acc = None
    for e in range(n_e):
        side, i = divmod(e, n_e // 2)
        here = slice(i * f_dev, (i + 1) * f_dev)
        rows = slice(e * f_dev, (e + 1) * f_dev)
        g = g_acc[rows] + lax.dot_general((g_in0, g_in1)[side][here], x[...], NT, preferred_element_type=jnp.float32)
        if e == n_e // 2:
            made.wait()
        u = u_acc[rows] + lax.dot_general((u_in0, u_in1)[side][here], x[...], NT, preferred_element_type=jnp.float32)
        h = (g / (1.0 + jnp.exp(-g)) * u * mix_t[e : e + 1, :]).astype(jnp.bfloat16)
        pick = jnp.where(slots == pos_t[e : e + 1, :], 1.0, 0.0).astype(jnp.bfloat16)
        part = lax.dot_general(pick, h, NT, preferred_element_type=jnp.float32)
        acc = part if acc is None else acc + part
    packed[...] = acc.astype(jnp.bfloat16)


class Rows:
    def __init__(self, at, w, buf, sems, first, f_dev):
        self.at, self.w, self.buf, self.sems, self.f_dev = at, w, buf, sems, f_dev
        self.blocks = COLS[first : first + buf.shape[1] // f_dev]

    def each(self, act):
        def one(e, carry):
            for j, off in enumerate(self.blocks):
                row = pl.multiple_of((self.at[0] ^ off) * self.f_dev, 128)
                dst = self.buf.at[e, j * self.f_dev : (j + 1) * self.f_dev, :]
                act(pltpu.make_async_copy(self.w.at[e, pl.ds(row, self.f_dev), :], dst, self.sems.at[e, j]))
            return carry

        lax.fori_loop(0, self.buf.shape[0], one, 0)


def fetch_kernel(at, wd, buf, sems, *, first, f_dev):
    rows = Rows(at, wd, buf, sems, first, f_dev)
    rows.each(lambda c: c.start())
    rows.each(lambda c: c.wait())


def down(acc, blocks, pos, w, unroll):
    cap, _ = blocks[0].shape
    rows, lanes = acc.shape[0], pos.shape[1]
    slots = lax.broadcasted_iota(jnp.int32, (rows, lanes), 1).astype(jnp.float32)

    def one(e, carry):
        here = pos[pl.ds(pl.multiple_of(e * rows, rows), rows), :]
        place = [jnp.where(slots + float(lo) == here, 1.0, 0.0) for lo in range(0, cap, lanes)]
        place = jnp.concatenate(place, axis=1)[:, :cap].astype(jnp.bfloat16)
        h = [jnp.dot(place, b[...], preferred_element_type=jnp.float32).astype(jnp.bfloat16) for b in blocks]
        acc[...] += jnp.dot(jnp.concatenate(h, axis=1), w[e], preferred_element_type=jnp.float32)
        return carry

    lax.fori_loop(0, w.shape[0], one, 0, unroll=unroll)


def down_a_kernel(at, *refs):
    blocks, (pos, w, wd, acc, buf, sems) = refs[:EARLY], refs[EARLY:]
    rows = Rows(at, wd, buf, sems, EARLY, blocks[0].shape[1])
    rows.each(lambda c: c.start())
    acc[...] = jnp.zeros(acc.shape, acc.dtype)
    down(acc, blocks, pos, w, 1)
    rows.each(lambda c: c.wait())


def down_b_kernel(*refs):
    late = len(COLS) - EARLY
    blocks, (pos, w2, acc, out) = refs[:late], refs[late:]
    out[...] = acc[...]
    down(out, blocks, pos, w2, 2)


def planned(tokens, routes, gates, w_gate, w_up, w_down):
    n_tok, d_dev = tokens.shape
    n_e, f_dev, _ = w_gate.shape
    rows, n = 4 * n_tok, len(COLS)
    experts = n_e * lax.axis_size("expert")
    bf16, f32, dma = jnp.bfloat16, jnp.float32, pltpu.SemaphoreType.DMA
    at = jnp.stack([lax.axis_index("tensor"), lax.axis_index("expert")]).astype(jnp.int32)
    sizes = dict(n_e=n_e, f_dev=f_dev, width=d_dev)
    mid, k_half = n_e // 2, len(HERE) * d_dev
    whole, part = ((n_e * f_dev, k_half), bf16), ((mid * f_dev, k_half), bf16)
    whole_sems, part_sems = dma((n_e, len(HERE))), dma((mid, len(HERE)))
    sums = ((n_e * f_dev, rows), f32)
    half = pltpu.VMEM((rows, len(HERE) * d_dev), bf16)
    caps = [c for c in CAPS if c < n_e * rows] + [n_e * rows]

    tok, mix = call(
        pre_kernel, [HBM] * 3, [((n_tok, d_dev), bf16), ((experts, d_dev), bf16)],
        [pltpu.VMEM(routes.T.shape, jnp.int32), pltpu.VMEM(gates.T.shape, bf16), dma((3,))],
        4, tokens, routes.T, gates.T,
    )
    z2, z4, z6 = (swap(tokens, "tensor", k) for k in (2, 4, 6))

    def load(jobs):
        shapes = [whole if hi - lo == n_e else part for _, (lo, hi), _ in jobs]
        sems = [whole_sems if hi - lo == n_e else part_sems for _, (lo, hi), _ in jobs]
        body = functools.partial(load_kernel, jobs=jobs, width=d_dev)
        return call(body, [SMEM, HBM, HBM], shapes, sems, 4, at, w_gate, w_up)

    g_a, u_a0 = load(((0, (0, n_e), HERE), (1, (0, mid), HERE)))
    line = jnp.concatenate([tok, z2, z4, z6, mix], axis=0)
    line_x = swap(line, "expert", 2)
    line_y = swap(line[:rows], "tensor", 1)
    u_a1, g_b0 = load(((1, (mid, n_e), HERE), (0, (0, mid), BESIDE)))
    side_1 = swap(line_x[: rows // 2], "tensor", 1)
    side_2 = swap(line_y[rows // 2 :], "expert", 2)
    mine_a = jnp.concatenate([line, line_x], axis=0)
    other_a = swap(mine_a, "expert", 1)
    x_a, g_acc, mix_t, pos_t, pos_c, taken, g_b1 = call(
        functools.partial(early_g_kernel, n_tok=n_tok, caps=caps[:-1], **sizes),
        [SMEM, VMEM, VMEM, VMEM, HBM],
        [(half.shape, bf16), sums, ((n_e, rows), f32), ((n_e, rows), f32), ((n_e * rows, 128), f32), ((1,), jnp.int32), part],
        [pltpu.VMEM((128, rows), f32), part_sems],
        8, at, mine_a, other_a, g_a, w_gate,
    )
    mine_b = jnp.concatenate([line_y, side_1, side_2], axis=0)
    other_b = swap(mine_b, "expert", 1)
    u_acc, u_b0 = call(
        functools.partial(early_u_kernel, **sizes),
        [SMEM, VMEM, VMEM, VMEM, HBM], [sums, part], [part_sems], 8, at, x_a, u_a0, u_a1, w_up,
    )
    (packed,) = call(
        functools.partial(late_kernel, n_tok=n_tok, **sizes),
        [SMEM] + [VMEM] * 5 + [HBM] + [VMEM] * 4, [((n_e * rows, f_dev), bf16)],
        [half, pltpu.VMEM(part[0], bf16), part_sems], 12,
        at, mine_b, other_b, g_b0, g_b1, u_b0, w_up, g_acc, u_acc, mix_t, pos_t,
    )

    def finish(cap, packed, pos_c, w_down, at):
        hidden = packed[:cap]
        (w,) = call(
            functools.partial(fetch_kernel, first=0, f_dev=f_dev),
            [SMEM, HBM], [((n_e, EARLY * f_dev, d_dev), bf16)], [dma((n_e, EARLY))], 4, at, w_down,
        )
        h1 = swap(hidden, "tensor", 1)
        h2, h4 = (swap(hidden, "tensor", k) for k in (2, 4))
        h3, h5 = (swap(h, "tensor", 1) for h in (h2, h4))
        h6, h7 = (swap(h, "tensor", 2) for h in (h4, h5))
        acc, w2 = call(
            down_a_kernel, [SMEM] + [VMEM] * (EARLY + 2) + [HBM],
            [((rows, d_dev), f32), ((n_e, (n - EARLY) * f_dev, d_dev), bf16)], [dma((n_e, n - EARLY))], 16,
            at, hidden, h1, h2, h4, h3, h5, pos_c, w, w_down,
        )
        return call(down_b_kernel, [VMEM] * (n - EARLY + 3), [((rows, d_dev), f32)], [], 16, h6, h7, pos_c, w2, acc)[0]

    summed = lax.switch(taken[0], [functools.partial(finish, c) for c in caps], packed, pos_c, w_down, at)
    total = summed[:n_tok]
    for j, k in enumerate(ROWS[1:], 1):
        piece = swap(summed[j * n_tok : (j + 1) * n_tok].astype(bf16), "expert", k)
        total = total + piece.astype(f32)
    return total.astype(bf16)


def on_device(*args):
    tokens, _, _, w_gate, _, _ = args
    n_e, n_t = lax.axis_size("expert"), lax.axis_size("tensor")
    fits = (n_e, n_t) == (4, 8) and n_e * tokens.shape[0] == CAP
    tiled = w_gate.shape[0] % 2 == 0 and tokens.shape[0] % 16 == 0 and tokens.shape[1] % 128 == 0 and w_gate.shape[1] % 128 == 0
    if not (fits and tiled):
        return general(*args)
    return planned(*args)


def solution(mesh):
    placed = (
        P("expert", "tensor"),
        P("expert", None),
        P("expert", None),
        P("expert", "tensor", None),
        P("expert", "tensor", None),
        P("expert", None, "tensor"),
    )
    return jax.shard_map(
        on_device, mesh=mesh, in_specs=placed, out_specs=P("expert", "tensor"), check_vma=False
    )
```
